32 devices in a mesh: row: 4 (over x, core), col: 8 (over z, y).
Axes of the slice: x: 2, y: 2, z: 4, core: 2. Of those that a mesh axis runs over, the one named last changes fastest.
Arguments:
- matrix: float32 [2048, 2048], P('row', 'col'), as said below
- start_vectors: float32 [2048, 512], P(('col', 'row')), may hold values from -6 to 6
- interval: float32 [2], replicated, as said below
Outputs:
- ortho_basis: float32 [2048, 512], P(('col', 'row'))
- projected: float32 [512, 512], replicated
- residual: float32 [2048, 512], P(('col', 'row'))
The draws below stay inside these ranges and needn't reach their ends.
Inputs may be any that keep to these rules, and one draw needn't show every extreme that they name: matrix is exactly symmetric (entry (r, c) equals entry (c, r)); its eigenvalues lie within about -1.45 to 1.45. interval[0] lies in [-1.2, -0.7] and interval[1] in [1.45, 1.9].
All inputs are finite; a program needn't handle non-finite values.
Results may differ from the reference program's by a relative error of at most 0.0003.
Values sent between devices are 32-bit elements.
A program may use at most 128 MiB of HBM per device.

```python
import math
import jax
import jax.numpy as jnp
from jax import lax

K = 512
FILTER_DEG = 3
OUTER = 2
N = 2048


def draw_matrix(key, part):
    entries = jax.random.normal(key, (N, N), jnp.float32)
    return ((entries + entries.T) * (0.5 / math.sqrt(N))).astype(jnp.float32)


def draw_interval(key, part):
    low_key = jax.random.fold_in(key, 11)
    high_key = jax.random.fold_in(key, 23)
    low_end = jax.random.uniform(low_key, (), jnp.float32, -1.2, -0.7)
    high_end = jax.random.uniform(high_key, (), jnp.float32, 1.45, 1.9)
    return jnp.stack([low_end, high_end]).astype(jnp.float32)


def shard_levels(rng, extent, split, least, high):
    def one(axis_at, blocks):
        steps = jax.random.uniform(jax.random.fold_in(jax.random.fold_in(rng, 6), axis_at), (blocks,), jnp.float32, least / len(split), high / len(split))
        return jnp.repeat(jnp.exp(steps), extent[axis_at] // blocks).reshape((-1,) + (1,) * (len(extent) - axis_at - 1))

    gain = one(*split[0])
    for cut in split[1:]:
        gain = gain * one(*cut)
    return gain


def gaussian(rng, extent, deviation, limit, cuts=(), kind=jnp.bfloat16):
    values = jax.random.normal(rng, extent, jnp.float32) * deviation
    if len(cuts) > 0:
        values = shard_levels(rng, extent, cuts, -0.22, 0.18) * values
    return jnp.clip(values, min=-limit, max=limit).astype(kind)


def setup_inputs(seed: int = 0) -> dict:
    keys = jax.random.split(jax.random.key(seed), 4)
    matrix = draw_matrix(jax.random.fold_in(keys[3], 71), 0)
    start_vectors = gaussian(keys[1], (N, K), 1.0, 6.0, ((0, 32),), jnp.float32)
    interval = draw_interval(jax.random.fold_in(keys[3], 71), 0)
    return dict(matrix=matrix, start_vectors=start_vectors, interval=interval)


def product(left, right):
    return jnp.dot(left, right, precision=lax.Precision.HIGHEST, preferred_element_type=jnp.float32)


def tri_solve(factor, values):
    return jax.scipy.linalg.solve_triangular(factor, values, lower=True)


def reference(matrix, start_vectors, interval):
    center = 0.5 * (interval[0] + interval[1])
    half_width = 0.5 * (interval[1] - interval[0])
    total_rows = matrix.shape[0]
    positions = lax.iota(jnp.int32, total_rows)
    diagonal = positions[:, None] == positions[None, :]
    operator = jnp.where(diagonal, matrix - center, matrix) / half_width
    current_start = start_vectors
    for sweep_index in range(OUTER):
        previous = current_start
        current = product(operator, current_start)
        for degree in range(2, FILTER_DEG + 1):
            previous, current = current, 2.0 * product(operator, current) - previous
        mapped = product(operator, current)
        gram_matrix = product(current.T, current) / total_rows
        cross_terms = product(current.T, mapped) / total_rows
        factor = jnp.linalg.cholesky(gram_matrix)
        ortho_basis = tri_solve(factor, current.T).T
        partial_value = tri_solve(factor, cross_terms)
        projected = tri_solve(factor, partial_value.T).T
        current_start = ortho_basis
    residual = tri_solve(factor, mapped.T).T - product(ortho_basis, projected)
    return ortho_basis, projected, residual
```

```python
import functools

import jax
import jax.numpy as jnp
from jax import lax
from jax.experimental import pallas as pl
from jax.experimental.pallas import tpu as pltpu
from jax.sharding import PartitionSpec as P

FILTER_DEG = 3
OUTER = 2
PANEL = 8


def product(left, right, precision=lax.Precision.HIGHEST):
    return jnp.dot(left, right, precision=precision, preferred_element_type=jnp.float32)


def contract(left, right, left_dim, right_dim):
    return lax.dot_general(
        left,
        right,
        (((left_dim,), (right_dim,)), ((), ())),
        precision=lax.Precision.HIGHEST,
        preferred_element_type=jnp.float32,
    )


def factor_panel(panel, first):
    rows = panel.shape[0]
    row_at = lax.broadcasted_iota(jnp.int32, panel.shape, 0)
    pivots = jnp.ones((rows, 1), jnp.float32)
    pivot_at = lax.broadcasted_iota(jnp.int32, (rows, 1), 0)
    for step in range(rows):
        column = panel[:, first + step : first + step + 1]
        pivot = column[step : step + 1, :]
        pivots = jnp.where(pivot_at == step, pivot, pivots)
        if step < rows - 1:
            multiplier = column / pivot
            change = multiplier * panel[step : step + 1, :]
            panel = jnp.where(row_at > step, panel - change, panel)
    return panel * lax.rsqrt(pivots)


def factor_kernel(block, gram_ref, inverse_ref, work, tile):
    order = gram_ref.shape[0]
    work[...] = gram_ref[...]
    at_row = lax.broadcasted_iota(jnp.int32, (order, order), 0)
    at_col = lax.broadcasted_iota(jnp.int32, (order, order), 1)
    inverse_ref[...] = (at_row == at_col).astype(jnp.float32)
    unit = (
        lax.broadcasted_iota(jnp.int32, (block, block), 0)
        == lax.broadcasted_iota(jnp.int32, (block, block), 1)
    ).astype(jnp.float32)
    for start in range(0, order, block):
        stop = start + block
        tile[:, :block] = work[start:stop, start:stop]
        tile[:, block:] = unit
        for first in range(0, block, PANEL):
            last = first + PANEL
            done = factor_panel(tile[first:last, :], first)
            tile[first:last, :] = done
            if last < block:
                tile[last:, :] -= contract(done[:, :block], done, 0, 0)[last:, :]
        small = tile[:, block:]
        solved = product(small, inverse_ref[start:stop, :])
        inverse_ref[start:stop, :] = solved
        if stop < order:
            below = contract(work[stop:, start:stop], small, 1, 1)
            work[stop:, stop:] -= contract(below, below, 1, 1)
            inverse_ref[stop:, :] -= product(below, solved)
    inverse_ref[...] = jnp.where(at_row >= at_col, inverse_ref[...], 0.0)


def inverse_factor(gram_matrix):
    order = gram_matrix.shape[0]
    block = min(128, order)
    return pl.pallas_call(
        functools.partial(factor_kernel, block),
        out_shape=jax.ShapeDtypeStruct((order, order), jnp.float32),
        in_specs=[pl.BlockSpec(memory_space=pltpu.VMEM)],
        out_specs=pl.BlockSpec(memory_space=pltpu.VMEM),
        scratch_shapes=[
            pltpu.VMEM((order, order), jnp.float32),
            pltpu.VMEM((block, 2 * block), jnp.float32),
        ],
        cost_estimate=pl.CostEstimate(flops=2 * order**3, bytes_accessed=8 * order**2, transcendentals=order),
    )(gram_matrix)


def on_device(matrix, start_vectors, interval):
    block_rows = matrix.shape[0]
    slab_rows, vectors = start_vectors.shape
    row_count, col_count = lax.axis_size("row"), lax.axis_size("col")
    total_rows = slab_rows * row_count * col_count
    width = vectors // col_count
    row_index = lax.axis_index("row")
    center = 0.5 * (interval[0] + interval[1])
    half_width = 0.5 * (interval[1] - interval[0])

    strip = lax.all_gather(matrix, "col", axis=1, tiled=True)
    global_rows = row_index * block_rows + lax.iota(jnp.int32, block_rows)
    diagonal = global_rows[:, None] == lax.iota(jnp.int32, total_rows)[None, :]
    shifted = jnp.where(diagonal, strip - center, strip) / half_width

    def apply(group):
        return lax.all_gather(product(shifted, group, lax.Precision.HIGH), "row", axis=0, tiled=True)

    def to_group(slab):
        mine = lax.all_to_all(slab, "col", split_axis=1, concat_axis=0, tiled=True)
        every = lax.all_gather(mine.reshape(col_count, slab_rows, width), "row", axis=1)
        return every.reshape(total_rows, width)

    def to_slab(group):
        parts = group.reshape(col_count, row_count, slab_rows, width)
        mine = lax.dynamic_index_in_dim(parts, row_index, 1, keepdims=False)
        return lax.all_to_all(mine.reshape(col_count * slab_rows, width), "col", split_axis=0, concat_axis=1, tiled=True)

    def filtered(group):
        previous, current = group, apply(group)
        for degree in range(2, FILTER_DEG + 1):
            previous, current = current, 2.0 * apply(current) - previous
        return current

    group = to_group(start_vectors)
    inverses = []

    def normalised(slab):
        for inverse in inverses:
            slab = contract(slab, inverse, 1, 1)
        return slab

    for sweep_index in range(OUTER):
        group = filtered(group)
        slab = normalised(to_slab(group))
        if sweep_index == OUTER - 1:
            mapped = normalised(to_slab(apply(group)))
            pair = jnp.concatenate([slab, mapped], axis=1)
            sums = lax.psum(contract(slab, pair, 0, 0), ("row", "col")) / total_rows
            gram, cross = sums[:, :vectors], sums[:, vectors:]
        else:
            gram = lax.psum(contract(slab, slab, 0, 0), ("row", "col")) / total_rows
        inverses.append(inverse_factor(gram))
    inverse = inverses[-1]
    basis = contract(slab, inverse, 1, 1)
    projected = contract(product(inverse, cross), inverse, 1, 1)
    residual = contract(mapped, inverse, 1, 1) - product(basis, projected)
    return basis, projected, residual


def solution(mesh):
    return jax.shard_map(
        on_device,
        mesh=mesh,
        in_specs=(P("row", "col"), P(("col", "row"), None), P()),
        out_specs=(P(("col", "row"), None), P(), P(("col", "row"), None)),
        check_vma=False,
    )
```
